32 devices in a mesh: gx: 2 (over x), gy: 4 (over y, core), gz: 4 (over z).
Axes of the slice: x: 2, y: 2, z: 4, core: 2. Of those that a mesh axis runs over, the one named last changes fastest.
Arguments:
- right_side: float32 [4, 5, 2, 32, 512], P(None, None, 'gx', 'gy', 'gz'), may hold values from -6 to 6
- jacobian: bfloat16 [27, 5, 5, 2, 32, 512], P(None, None, None, 'gx', 'gy', 'gz'), may hold values from -0.14 to 12.14, as said below
Outputs:
- solution: float32 [4, 5, 2, 32, 512], P(None, None, 'gx', 'gy', 'gz')
- residual: float32 [4, 5, 2, 32, 512], P(None, None, 'gx', 'gy', 'gz')
The draws below stay inside these ranges and needn't reach their ends.
Inputs may be any that keep to these rules, and one draw needn't show every extreme that they name: `jacobian`: blocks of offsets other than 13 and the off-diagonal entries of block 13 lie within -0.14 to 0.14; the diagonal entries of block 13 exceed 5.8 in every cell.
All inputs are finite; a program needn't handle non-finite values.
Results may differ from the reference program's by a relative error of at most 0.0003.
Values sent between devices are 32-bit elements.
No kernel may reach another device: no remote copies, remote signals or barrier semaphores. Data moves between devices by JAX's collectives and lax.ppermute only.
A program may use at most 64 MiB of HBM per device.

```python
import jax
import jax.numpy as jnp
from jax import lax

COMP = 5
RHS = 4
STENCIL = 27
ITERS = 3
NX = 2
NY = 32
NZ = 512


def draw_jacobian(key, part):
    first_key, second_key = jax.random.split(jax.random.fold_in(key, 17))
    full_shape = (STENCIL, COMP, COMP, NX, NY, NZ)
    diag_shape = (COMP, NX, NY, NZ)
    entries = jax.random.uniform(first_key, full_shape, jnp.float32, -0.14, 0.14)
    diagonal = jax.random.uniform(second_key, diag_shape, jnp.float32, 6.0, 12.0)
    identity = jnp.eye(COMP, dtype=jnp.float32)[:, :, None, None, None]
    center = entries[13] + identity * diagonal[:, None]
    entries = entries.at[13].set(center)
    return entries.astype(jnp.bfloat16)


def levels(rng, extent, shards, least, high):
    level = 1.0
    for axis_at, blocks in shards:
        heights = jax.random.uniform(jax.random.fold_in(jax.random.fold_in(rng, 6), axis_at), (blocks,), jnp.float32, least / len(shards), high / len(shards))
        level = level * jnp.repeat(jnp.exp(heights), extent[axis_at] // blocks).reshape((-1,) + (1,) * (len(extent) - 1 - axis_at))
    return level


def noise(rng, extent, deviation, bound, shards=(), kind=jnp.bfloat16):
    array = jax.random.normal(rng, extent, jnp.float32) * deviation
    if len(shards) > 0:
        array = levels(rng, extent, shards, -0.22, 0.18) * array
    return jnp.clip(array, min=-bound, max=bound).astype(kind)


def setup_inputs(seed: int = 0) -> dict:
    streams_of = jax.random.split(jax.random.key(seed), 3)
    return {
        "right_side": noise(streams_of[0], (RHS, COMP, NX, NY, NZ), 1.0, 6.0, ((2, 2), (3, 4), (4, 4)), jnp.float32),
        "jacobian": draw_jacobian(jax.random.fold_in(streams_of[2], 71), 0),
    }


def dot_high(left, right):
    return jnp.dot(left.astype(jnp.float32), right.astype(jnp.float32), precision=lax.Precision.HIGHEST, preferred_element_type=jnp.float32)

def lower_solve(factor, target):
    solved = []
    for row_pos in range(factor.shape[0]):
        accum = target[row_pos]
        for prior in range(row_pos):
            accum = accum - factor[row_pos, prior] * solved[prior]
        solved.append(accum / factor[row_pos, row_pos])
    return jnp.stack(solved)

def upper_solve(factor, target):
    size_all = factor.shape[0]
    solved = [None] * size_all
    for row_pos in range(size_all - 1, -1, -1):
        accum = target[row_pos]
        for later in range(row_pos + 1, size_all):
            accum = accum - factor[later, row_pos] * solved[later]
        solved[row_pos] = accum / factor[row_pos, row_pos]
    return jnp.stack(solved)

def extend(field):
    padded = jnp.pad(field, ((0, 0), (0, 0), (1, 1), (1, 1), (0, 0)), mode='wrap')
    return jnp.pad(padded, ((0, 0), (0, 0), (0, 0), (0, 0), (1, 1)))

def apply_operator(jacobian, padded):
    extent_x = padded.shape[2] - 2
    extent_y = padded.shape[3] - 2
    extent_z = padded.shape[4] - 2
    total = jnp.zeros((padded.shape[0], padded.shape[1], extent_x, extent_y, extent_z), jnp.float32)
    for stencil_pos in range(27):
        start_x = stencil_pos // 9
        start_y = stencil_pos // 3 % 3
        start_z = stencil_pos % 3
        piece = padded[:, :, start_x:start_x + extent_x, start_y:start_y + extent_y, start_z:start_z + extent_z]
        block = jacobian[stencil_pos].astype(jnp.float32)
        for source_comp in range(block.shape[1]):
            total = total + block[None, :, source_comp] * piece[:, source_comp][:, None]
    return total

def reference(right_side, jacobian):
    field_shape = right_side.shape
    rhs_count = field_shape[0]
    flat_rhs = right_side.reshape(rhs_count, -1)
    start_factor = jnp.linalg.cholesky(dot_high(flat_rhs, flat_rhs.T))
    basis = [lower_solve(start_factor, flat_rhs)]
    hessen_rows = []
    for iteration in range(ITERS):
        workspace = apply_operator(jacobian, extend(basis[-1].reshape(field_shape))).reshape(rhs_count, -1)
        stacked = jnp.concatenate(basis, axis=0)
        coefficients = dot_high(stacked, workspace.T)
        workspace = workspace - dot_high(coefficients.T, stacked)
        factor = jnp.linalg.cholesky(dot_high(workspace, workspace.T))
        basis.append(lower_solve(factor, workspace))
        filler = jnp.zeros((rhs_count, rhs_count * (ITERS - iteration - 1)), jnp.float32)
        hessen_rows.append(jnp.concatenate([coefficients.T, factor, filler], axis=1))
    hessen = jnp.concatenate(hessen_rows, axis=0)
    target = jnp.concatenate([start_factor, jnp.zeros((rhs_count, rhs_count * ITERS), jnp.float32)], axis=1)
    normal_factor = jnp.linalg.cholesky(dot_high(hessen, hessen.T))
    middle = lower_solve(normal_factor, dot_high(hessen, target.T))
    weights = upper_solve(normal_factor, middle)
    solution = dot_high(weights.T, jnp.concatenate(basis[:-1], axis=0))
    solution_field = solution.reshape(field_shape)
    residual = right_side - apply_operator(jacobian, extend(solution_field))
    return (solution_field, residual)
```

```python
import functools

import jax
import jax.numpy as jnp
from jax import lax
from jax.experimental import pallas as pl
from jax.experimental.pallas import tpu as pltpu
from jax.sharding import PartitionSpec as P

STEPS = 3
CENTRE = 8.97
GROUP = 8
AXES = ("gx", "gy", "gz")

VMEM = pl.BlockSpec(memory_space=pltpu.VMEM)


def call(body, outs, operands, scratch=(), flops=100_000):
    moved = sum(o.size * 4 for o in outs) + sum(o.size * o.dtype.itemsize for o in operands)
    return pl.pallas_call(
        body,
        out_shape=outs,
        in_specs=[VMEM] * len(operands),
        out_specs=[VMEM] * len(outs),
        scratch_shapes=list(scratch),
        compiler_params=pltpu.CompilerParams(vmem_limit_bytes=24 * 1024 * 1024),
        cost_estimate=pl.CostEstimate(flops=flops, bytes_accessed=moved, transcendentals=0),
    )(*operands)


def shape(*dims):
    return jax.ShapeDtypeStruct(dims, jnp.float32)


def lane_ids(rows, lanes):
    return lax.broadcasted_iota(jnp.int32, (rows, lanes), 1)


def edge_tile(main, comp, rhs, comps, rows, lanes):
    lane = lane_ids(rows, lanes)
    place = lane % GROUP
    tile = jnp.zeros((rows, lanes), jnp.float32)
    for r in range(rhs):
        value = main(r * comps + comp)
        low = pltpu.roll(value, (r * GROUP + 3) % lanes, 1)
        high = pltpu.roll(value, (r * GROUP + 5) % lanes, 1)
        here = lane // GROUP == r
        tile = jnp.where(here & (place < 4), low, jnp.where(here, high, tile))
    return tile


def edges_kernel(rhs, comps, main_ref, edge_ref):
    _, rows, lanes = main_ref.shape
    for comp in range(comps):
        edge_ref[comp] = edge_tile(lambda i: main_ref[i], comp, rhs, comps, rows, lanes)


def blocks_kernel(layers, raw_ref, out_ref):
    def body(i, carry):
        own = raw_ref[9 + i].astype(jnp.float32)
        below = raw_ref[i].astype(jnp.float32)
        above = raw_ref[18 + i].astype(jnp.float32)
        out_ref[i] = own
        if layers == 2:
            out_ref[9 + i] = below + above
        else:
            out_ref[9 + i] = below
            out_ref[18 + i] = above
        return carry

    lax.fori_loop(0, 9, body, 0)


def assemble_kernel(rhs, comps, main_ref, edge_ref, first_ref, second_ref, out_ref):
    fields, rows, lanes = main_ref.shape
    even = lax.axis_index("gz") % 2 == 0
    place = lane_ids(rows, lanes) % GROUP
    for i in range(fields):
        out_ref[i] = main_ref[i]
    for comp in range(comps):
        one, two = first_ref[comp], second_ref[comp]
        above = jnp.where(even, one, two)
        below = jnp.where(even, two, one)
        ghost = jnp.where(place < 3, below, jnp.where(place > 4, above, edge_ref[comp]))
        out_ref[fields + comp] = ghost


def rows_kernel(layers, tiles, rows, *refs):
    ins, (first_ref, second_ref) = refs[:layers], refs[layers:]
    even = lax.axis_index("gy") % 2 == 0
    first_ref[...] = jnp.zeros_like(first_ref)
    second_ref[...] = jnp.zeros_like(second_ref)
    for layer in range(layers):
        head = ins[layer][pl.ds(0, tiles, stride=rows), :]
        tail = ins[layer][pl.ds(rows - 1, tiles, stride=rows), :]
        where = pl.ds(layer * tiles, tiles)
        first_ref[where, :] = jnp.where(even, tail, head)
        second_ref[where, :] = jnp.where(even, head, tail)


def operator_kernel(layers, rhs, comps, last, *refs):
    blocks_ref, first_ref, second_ref = refs[:3]
    field_refs = refs[3 : 3 + layers]
    fields = rhs * comps
    tiles, rows, lanes = field_refs[0].shape
    if last:
        early_refs = refs[3 + layers : -4]
        out_ref, gram_ref, moved_ref, pairs_ref = refs[-4:]
    else:
        product_ref, next_ref, edge_ref, moved_ref = refs[3 + layers :]

    even = lax.axis_index("gy") % 2 == 0
    sub = lax.broadcasted_iota(jnp.int32, (rows, lanes), 0)
    lane = lane_ids(rows, lanes)
    for layer in range(layers):
        for dy in range(3):
            def moved(tile):
                value = field_refs[layer][tile]
                if dy == 1:
                    return value
                at = layer * tiles + tile
                one = first_ref[pl.ds(at, 1), :]
                two = second_ref[pl.ds(at, 1), :]
                if dy == 2:
                    row = jnp.where(even, one, two)
                    return jnp.where(sub == rows - 1, row, pltpu.roll(value, rows - 1, 0))
                row = jnp.where(even, two, one)
                return jnp.where(sub == 0, row, pltpu.roll(value, 1, 0))

            for comp in range(comps):
                ghost = moved(fields + comp)
                for r in range(rhs):
                    tile = r * comps + comp
                    value = moved(tile)
                    at = layer * 9 + dy * 3
                    left = pltpu.roll(ghost, (-(r * GROUP + 2)) % lanes, 1)
                    right = pltpu.roll(ghost, (lanes - 1 - (r * GROUP + 5)) % lanes, 1)
                    moved_ref[at, tile] = jnp.where(lane == 0, left, pltpu.roll(value, 1, 1))
                    moved_ref[at + 1, tile] = value
                    moved_ref[at + 2, tile] = jnp.where(
                        lane == lanes - 1, right, pltpu.roll(value, lanes - 1, 1)
                    )

    def body(at, total):
        total = list(total)
        for source in range(comps):
            values = [moved_ref[at, r * comps + source] for r in range(rhs)]
            for comp in range(comps):
                block = blocks_ref[at, comp * comps + source]
                for r in range(rhs):
                    total[r * comps + comp] += block * values[r]
        return tuple(total)

    zero = jnp.zeros((rows, lanes), jnp.float32)
    total = lax.fori_loop(0, 9 * layers, body, (zero,) * fields)
    if not last:
        for i in range(fields):
            product_ref[i] = total[i]
            next_ref[i] = total[i] - CENTRE * field_refs[0][i]
        for comp in range(comps):
            edge_ref[comp] = edge_tile(lambda i: next_ref[i], comp, rhs, comps, rows, lanes)
        return
    for i in range(fields):
        out_ref[i] = total[i]
    start_ref, products = early_refs[0], list(early_refs[1:]) + [out_ref]
    for at, (one, two) in enumerate(gram_pairs(rhs)):
        left = products[one // rhs] if one >= 0 else start_ref
        first = (one % rhs if one >= 0 else -1 - one) * comps
        second = two % rhs * comps
        accum = None
        for comp in range(comps):
            term = left[first + comp] * products[two // rhs][second + comp]
            accum = term if accum is None else accum + term
        pairs_ref[pl.ds(at * rows, rows), :] = accum
    count = len(gram_pairs(rhs))
    for at in range(count, pairs_ref.shape[0] // rows):
        pairs_ref[pl.ds(at * rows, rows), :] = zero
    slots = pairs_ref.shape[0] // rows
    sums = pairs_ref[pl.ds(0, slots, stride=rows), :]
    for row in range(1, rows):
        sums = sums + pairs_ref[pl.ds(row, slots, stride=rows), :]
    sums = jnp.sum(sums, axis=1, keepdims=True)
    diagonal = lax.broadcasted_iota(jnp.int32, (slots, slots), 0) == lane_ids(slots, slots)
    packed = jnp.sum(jnp.where(diagonal, sums, 0.0), axis=0, keepdims=True)
    gram_ref[...] = jnp.broadcast_to(packed, gram_ref.shape)


def gram_pairs(rhs):
    size = rhs * STEPS
    pairs = [(i, j) for i in range(size) for j in range(i, size)]
    return pairs + [(-1 - r, j) for r in range(rhs) for j in range(size)]


def finish_kernel(rhs, comps, sums_ref, start_ref, *refs):
    basis = [start_ref, *refs[: STEPS - 1]]
    products = refs[STEPS - 1 : 2 * STEPS - 1]
    solution_ref, residual_ref = refs[2 * STEPS - 1 :]
    _, rows, lanes = start_ref.shape
    size = rhs * STEPS
    packed = jnp.sum(sums_ref[...], axis=0, keepdims=True)
    gram, right = {}, {}
    for at, (one, two) in enumerate(gram_pairs(rhs)):
        entry = jnp.broadcast_to(packed[:, at : at + 1], (rows, lanes))
        if one >= 0:
            gram[one, two] = entry
        else:
            right[two, -1 - one] = entry
    inverse = []
    for k in range(size):
        inverse.append(1.0 / gram[k, k])
        for i in range(k + 1, size):
            factor = gram[k, i] * inverse[k]
            for j in range(i, size):
                gram[i, j] = gram[i, j] - factor * gram[k, j]
            for r in range(rhs):
                right[i, r] = right[i, r] - factor * right[k, r]
    for r in range(rhs):
        weights = [None] * size
        for k in range(size - 1, -1, -1):
            accum = right[k, r]
            for j in range(k + 1, size):
                accum = accum - gram[k, j] * weights[j]
            weights[k] = accum * inverse[k]
        for comp in range(comps):
            answer = None
            image = None
            for k in range(size):
                tile = k % rhs * comps + comp
                one = weights[k] * basis[k // rhs][tile]
                two = weights[k] * products[k // rhs][tile]
                answer = one if answer is None else answer + one
                image = two if image is None else image + two
            solution_ref[r * comps + comp] = answer
            residual_ref[r * comps + comp] = start_ref[r * comps + comp] - image


def paired(count, ring):
    first = [(i, i ^ 1) for i in range(count)]
    second = []
    for i in range(1, count - 1, 2):
        second += [(i, i + 1), (i + 1, i)]
    if ring and count > 2:
        second += [(count - 1, 0), (0, count - 1)]
    return first, second


def swap(value, axis, pairs):
    return lax.ppermute(value, axis, pairs)


def shards(sizes, right_side, jacobian):
    rhs, comps, _, rows, lanes = right_side.shape
    fields, tiles = rhs * comps, (rhs + 1) * comps
    layers = 2 if sizes["gx"] == 2 else 3
    devices = sizes["gx"] * sizes["gy"] * sizes["gz"]
    start = right_side.reshape(fields, rows, lanes)
    raw = jacobian.reshape(27, comps * comps, rows, lanes)

    (blocks,) = call(
        functools.partial(blocks_kernel, layers), [shape(9 * layers, comps * comps, rows, lanes)], [raw]
    )
    (edge,) = call(functools.partial(edges_kernel, rhs, comps), [shape(comps, rows, lanes)], [start])

    z_pairs = paired(sizes["gz"], False)
    y_pairs = paired(sizes["gy"], True)
    packed_rows = -(-layers * tiles // 8) * 8
    slots = -(-len(gram_pairs(rhs)) // 8) * 8
    moved = pltpu.VMEM((9 * layers, fields, rows, lanes), jnp.float32)

    basis, products = [start], []
    for step in range(STEPS):
        below, above = (swap(edge, "gz", pairs) for pairs in z_pairs)
        (field,) = call(
            functools.partial(assemble_kernel, rhs, comps),
            [shape(tiles, rows, lanes)],
            [basis[-1], edge, below, above],
        )
        count = sizes["gx"]
        if layers == 2:
            slabs = [field, swap(field, "gx", [(0, 1), (1, 0)])]
        else:
            slabs = [
                field,
                swap(field, "gx", [(i, (i + 1) % count) for i in range(count)]),
                swap(field, "gx", [((i + 1) % count, i) for i in range(count)]),
            ]
        flat = [slab.reshape(tiles * rows, lanes) for slab in slabs]
        sent = call(
            functools.partial(rows_kernel, layers, tiles, rows),
            [shape(packed_rows, lanes)] * 2,
            flat,
        )
        first, second = (swap(value, "gy", pairs) for value, pairs in zip(sent, y_pairs))
        last = step == STEPS - 1
        flops = 2 * 9 * layers * comps * fields * rows * lanes
        if last:
            product, gram = call(
                functools.partial(operator_kernel, layers, rhs, comps, True),
                [shape(fields, rows, lanes), shape(devices, slots)],
                [blocks, first, second, *slabs, start, *products],
                [moved, pltpu.VMEM((slots * rows, lanes), jnp.float32)],
                flops,
            )
            products.append(product)
        else:
            product, following, edge = call(
                functools.partial(operator_kernel, layers, rhs, comps, False),
                [shape(fields, rows, lanes), shape(fields, rows, lanes), shape(comps, rows, lanes)],
                [blocks, first, second, *slabs],
                [moved],
                flops,
            )
            products.append(product)
            basis.append(following)

    sums = lax.all_to_all(gram, AXES, 0, 0, tiled=True)
    answer, residual = call(
        functools.partial(finish_kernel, rhs, comps),
        [shape(fields, rows, lanes)] * 2,
        [sums, *basis, *products],
    )
    return answer.reshape(right_side.shape), residual.reshape(right_side.shape)


def solution(mesh):
    cells = P(None, None, "gx", "gy", "gz")
    return jax.shard_map(
        functools.partial(shards, dict(mesh.shape)),
        mesh=mesh,
        in_specs=(cells, P(None, None, None, "gx", "gy", "gz")),
        out_specs=(cells, cells),
        check_vma=False,
    )
```

```python
import functools

import jax
import jax.numpy as jnp
from jax import lax
from jax.experimental import pallas as pl
from jax.experimental.pallas import tpu as pltpu
from jax.sharding import PartitionSpec as P

STEPS = 3
CENTRE = 8.97
GROUP = 8
AXES = ("gx", "gy", "gz")

VMEM = pl.BlockSpec(memory_space=pltpu.VMEM)


def call(body, outs, operands, scratch=(), flops=100_000):
    moved = sum(o.size * 4 for o in outs) + sum(o.size * o.dtype.itemsize for o in operands)
    return pl.pallas_call(
        body,
        out_shape=outs,
        in_specs=[VMEM] * len(operands),
        out_specs=[VMEM] * len(outs),
        scratch_shapes=list(scratch),
        compiler_params=pltpu.CompilerParams(vmem_limit_bytes=24 * 1024 * 1024),
        cost_estimate=pl.CostEstimate(flops=flops, bytes_accessed=moved, transcendentals=0),
    )(*operands)


def shape(*dims):
    return jax.ShapeDtypeStruct(dims, jnp.float32)


def lane_ids(rows, lanes):
    return lax.broadcasted_iota(jnp.int32, (rows, lanes), 1)


def edge_tile(main, comp, rhs, comps, rows, lanes):
    lane = lane_ids(rows, lanes)
    place = lane % GROUP
    tile = jnp.zeros((rows, lanes), jnp.float32)
    for r in range(rhs):
        value = main(r * comps + comp)
        low = pltpu.roll(value, (r * GROUP + 3) % lanes, 1)
        high = pltpu.roll(value, (r * GROUP + 5) % lanes, 1)
        here = lane // GROUP == r
        tile = jnp.where(here & (place < 4), low, jnp.where(here, high, tile))
    return tile


def prepare_kernel(layers, rhs, comps, start_ref, raw_ref, blocks_ref, edge_ref, first_ref, second_ref, narrow_ref):
    _, rows, lanes = start_ref.shape
    size = comps * comps

    def widen(i, carry):
        own = raw_ref[9 + i].astype(jnp.float32)
        below = raw_ref[i].astype(jnp.float32)
        above = raw_ref[18 + i].astype(jnp.float32)
        blocks_ref[i] = own
        if layers == 2:
            blocks_ref[9 + i] = below + above
        else:
            blocks_ref[9 + i] = below
            blocks_ref[18 + i] = above
        return carry

    lax.fori_loop(0, 9, widen, 0)
    lane = lane_ids(rows, lanes)
    pair = lane % 4 < 2
    zero = jnp.zeros((rows, lanes), jnp.float32)

    def narrow(i, carry):
        tile = zero
        for at in range(size):
            tile = jnp.where(lane // 4 == at, pltpu.roll(blocks_ref[i, at], (at * 4 + 2) % lanes, 1), tile)
        narrow_ref[i] = tile
        return carry

    lax.fori_loop(0, 9 * layers, narrow, 0)
    if layers % 2:
        narrow_ref[9 * layers] = zero
    even = lax.axis_index("gz") % 2 == 0
    for comp in range(comps):
        tile = edge_tile(lambda i: start_ref[i], comp, rhs, comps, rows, lanes)
        edge_ref[comp] = tile
        first_ref[comp] = tile
        second_ref[comp] = tile
    for i in range(0, narrow_ref.shape[0], 2):
        one, two = narrow_ref[i], narrow_ref[i + 1]
        up = jnp.where(pair, one, pltpu.roll(two, 2, 1))
        down = jnp.where(pair, pltpu.roll(one, lanes - 2, 1), two)
        first_ref[comps + i // 2] = jnp.where(even, up, down)
        second_ref[comps + i // 2] = jnp.where(even, down, up)


def send_rows(field_ref, first_ref, second_ref, tiles, rows):
    even = lax.axis_index("gy") % 2 == 0
    head = field_ref[pl.ds(0, tiles, stride=rows), :]
    tail = field_ref[pl.ds(rows - 1, tiles, stride=rows), :]
    spare = first_ref.shape[0] - tiles
    if spare:
        empty = jnp.zeros((spare, first_ref.shape[1]), jnp.float32)
        first_ref[pl.ds(tiles, spare), :] = empty
        second_ref[pl.ds(tiles, spare), :] = empty
    first_ref[pl.ds(0, tiles), :] = jnp.where(even, tail, head)
    second_ref[pl.ds(0, tiles), :] = jnp.where(even, head, tail)


def assemble_kernel(rhs, comps, start_ref, edge_ref, first_ref, second_ref, out_ref, head_ref, tail_ref):
    fields, rows, lanes = start_ref.shape
    even = lax.axis_index("gz") % 2 == 0
    place = lane_ids(rows, lanes) % GROUP
    for i in range(fields):
        out_ref[pl.ds(i * rows, rows), :] = start_ref[i]
    for comp in range(comps):
        one, two = first_ref[comp], second_ref[comp]
        above = jnp.where(even, one, two)
        below = jnp.where(even, two, one)
        ghost = jnp.where(place < 3, below, jnp.where(place > 4, above, edge_ref[comp]))
        out_ref[pl.ds((fields + comp) * rows, rows), :] = ghost
    send_rows(out_ref, head_ref, tail_ref, fields + comps, rows)


def ghost_blocks_kernel(rhs, comps, first_ref, second_ref, out_ref):
    count, size, rows, lanes = out_ref.shape
    even = lax.axis_index("gz") % 2 == 0
    lane = lane_ids(rows, lanes)
    pair = lane % 4 < 2
    place = lane % GROUP
    column = jnp.where(place < 3, place - 1, place - 3)
    inner = (place == 1) | (place == 2) | (place == 5) | (place == 6)
    inner = inner & (lane < rhs * GROUP)
    for i in range(0, count, 2):
        one, two = first_ref[comps + i // 2], second_ref[comps + i // 2]
        above = jnp.where(even, one, two)
        below = jnp.where(even, two, one)
        tiles = [jnp.where(pair, below, pltpu.roll(above, 2, 1))]
        if i + 1 < count:
            tiles.append(jnp.where(pair, pltpu.roll(below, lanes - 2, 1), above))
        for at in range(size):
            index = jnp.where(inner, column + at * 4, lanes - 1)
            for k, tile in enumerate(tiles):
                out_ref[i + k, at] = jnp.take_along_axis(tile, index, axis=1)


def operator_kernel(layers, rhs, comps, last, *refs):
    fields, tiles = rhs * comps, (rhs + 1) * comps
    blocks_ref, refs = refs[0], refs[1:]
    if not last:
        ghosts_ref, refs = refs[0], refs[1:]
    field_refs, first_refs, second_refs = (refs[i * layers : (i + 1) * layers] for i in range(3))
    refs = refs[3 * layers :]
    rows, lanes = blocks_ref.shape[2:]
    if last:
        early_refs = refs[:-4]
        out_ref, gram_ref, moved_ref, pairs_ref = refs[-4:]
    else:
        product_ref, next_ref, head_ref, tail_ref, moved_ref = refs

    even = lax.axis_index("gy") % 2 == 0
    sub = lax.broadcasted_iota(jnp.int32, (rows, lanes), 0)
    lane = lane_ids(rows, lanes)
    for layer in range(layers):
        for dy in range(3):
            def moved(tile):
                value = field_refs[layer][pl.ds(tile * rows, rows), :]
                if dy == 1:
                    return value
                one = first_refs[layer][pl.ds(tile, 1), :]
                two = second_refs[layer][pl.ds(tile, 1), :]
                if dy == 2:
                    row = jnp.where(even, one, two)
                    return jnp.where(sub == rows - 1, row, pltpu.roll(value, rows - 1, 0))
                row = jnp.where(even, two, one)
                return jnp.where(sub == 0, row, pltpu.roll(value, 1, 0))

            at = layer * 9 + dy * 3
            for comp in range(comps):
                ghost = moved(fields + comp)
                if not last:
                    moved_ref[at, fields + comp] = pltpu.roll(ghost, 1, 1)
                    moved_ref[at + 1, fields + comp] = ghost
                    moved_ref[at + 2, fields + comp] = pltpu.roll(ghost, lanes - 1, 1)
                for r in range(rhs):
                    tile = r * comps + comp
                    value = moved(tile)
                    left = pltpu.roll(ghost, (-(r * GROUP + 2)) % lanes, 1)
                    right = pltpu.roll(ghost, (lanes - 1 - (r * GROUP + 5)) % lanes, 1)
                    moved_ref[at, tile] = jnp.where(lane == 0, left, pltpu.roll(value, 1, 1))
                    moved_ref[at + 1, tile] = value
                    moved_ref[at + 2, tile] = jnp.where(
                        lane == lanes - 1, right, pltpu.roll(value, lanes - 1, 1)
                    )

    def body(at, total):
        total = list(total)
        for source in range(comps):
            values = [moved_ref[at, r * comps + source] for r in range(rhs)]
            for comp in range(comps):
                block = blocks_ref[at, comp * comps + source]
                for r in range(rhs):
                    total[r * comps + comp] += block * values[r]
            if not last:
                value = moved_ref[at, fields + source]
                for comp in range(comps):
                    total[fields + comp] += ghosts_ref[at, comp * comps + source] * value
        return tuple(total)

    zero = jnp.zeros((rows, lanes), jnp.float32)
    total = lax.fori_loop(0, 9 * layers, body, (zero,) * (fields if last else tiles))
    if not last:
        main = []
        for i in range(fields):
            product_ref[i] = total[i]
            main.append(total[i] - CENTRE * field_refs[0][pl.ds(i * rows, rows), :])
            next_ref[pl.ds(i * rows, rows), :] = main[i]
        place = lane % GROUP
        own = (place == 3) | (place == 4)
        for comp in range(comps):
            where = pl.ds((fields + comp) * rows, rows)
            ghost = total[fields + comp] - CENTRE * field_refs[0][where, :]
            edge = edge_tile(lambda i: main[i], comp, rhs, comps, rows, lanes)
            next_ref[where, :] = jnp.where(own, edge, ghost)
        send_rows(next_ref, head_ref, tail_ref, tiles, rows)
        return
    for i in range(fields):
        out_ref[i] = total[i]
    start_ref, products = early_refs[0], list(early_refs[1:]) + [out_ref]
    for at, (one, two) in enumerate(gram_pairs(rhs)):
        left = products[one // rhs] if one >= 0 else start_ref
        first = (one % rhs if one >= 0 else -1 - one) * comps
        second = two % rhs * comps
        accum = None
        for comp in range(comps):
            term = left[first + comp] * products[two // rhs][second + comp]
            accum = term if accum is None else accum + term
        pairs_ref[pl.ds(at * rows, rows), :] = accum
    count = len(gram_pairs(rhs))
    for at in range(count, pairs_ref.shape[0] // rows):
        pairs_ref[pl.ds(at * rows, rows), :] = zero
    slots = pairs_ref.shape[0] // rows
    sums = pairs_ref[pl.ds(0, slots, stride=rows), :]
    for row in range(1, rows):
        sums = sums + pairs_ref[pl.ds(row, slots, stride=rows), :]
    sums = jnp.sum(sums, axis=1, keepdims=True)
    diagonal = lax.broadcasted_iota(jnp.int32, (slots, slots), 0) == lane_ids(slots, slots)
    packed = jnp.sum(jnp.where(diagonal, sums, 0.0), axis=0, keepdims=True)
    gram_ref[...] = jnp.broadcast_to(packed, gram_ref.shape)


def gram_pairs(rhs):
    size = rhs * STEPS
    pairs = [(i, j) for i in range(size) for j in range(i, size)]
    return pairs + [(-1 - r, j) for r in range(rhs) for j in range(size)]


def finish_kernel(rhs, comps, sums_ref, start_ref, *refs):
    products = refs[STEPS - 1 : 2 * STEPS - 1]
    solution_ref, residual_ref = refs[2 * STEPS - 1 :]
    _, rows, lanes = start_ref.shape
    size = rhs * STEPS

    def basis_tile(k, tile):
        if k < rhs:
            return start_ref[tile]
        return refs[k // rhs - 1][pl.ds(tile * rows, rows), :]

    packed = jnp.sum(sums_ref[...], axis=0, keepdims=True)
    gram, right = {}, {}
    for at, (one, two) in enumerate(gram_pairs(rhs)):
        entry = jnp.broadcast_to(packed[:, at : at + 1], (rows, lanes))
        if one >= 0:
            gram[one, two] = entry
        else:
            right[two, -1 - one] = entry
    inverse = []
    for k in range(size):
        inverse.append(1.0 / gram[k, k])
        for i in range(k + 1, size):
            factor = gram[k, i] * inverse[k]
            for j in range(i, size):
                gram[i, j] = gram[i, j] - factor * gram[k, j]
            for r in range(rhs):
                right[i, r] = right[i, r] - factor * right[k, r]
    for r in range(rhs):
        weights = [None] * size
        for k in range(size - 1, -1, -1):
            accum = right[k, r]
            for j in range(k + 1, size):
                accum = accum - gram[k, j] * weights[j]
            weights[k] = accum * inverse[k]
        for comp in range(comps):
            answer = None
            image = None
            for k in range(size):
                tile = k % rhs * comps + comp
                one = weights[k] * basis_tile(k, tile)
                two = weights[k] * products[k // rhs][tile]
                answer = one if answer is None else answer + one
                image = two if image is None else image + two
            solution_ref[r * comps + comp] = answer
            residual_ref[r * comps + comp] = start_ref[r * comps + comp] - image


def paired(count, ring):
    first = [(i, i ^ 1) for i in range(count)]
    second = []
    for i in range(1, count - 1, 2):
        second += [(i, i + 1), (i + 1, i)]
    if ring and count > 2:
        second += [(count - 1, 0), (0, count - 1)]
    return first, second


def across(count_x, step_x, pairs):
    count_y = len(pairs)
    return [
        (x * count_y + one, (x + step_x) % count_x * count_y + two) for x in range(count_x) for one, two in pairs
    ]


def shards(sizes, right_side, jacobian):
    rhs, comps, _, rows, lanes = right_side.shape
    fields, tiles = rhs * comps, (rhs + 1) * comps
    size = comps * comps
    layers = 2 if sizes["gx"] == 2 else 3
    count = 9 * layers
    devices = sizes["gx"] * sizes["gy"] * sizes["gz"]
    start = right_side.reshape(fields, rows, lanes)
    raw = jacobian.reshape(27, size, rows, lanes)

    z_pairs = paired(sizes["gz"], False)
    y_pairs = paired(sizes["gy"], True)
    still = [(i, i) for i in range(sizes["gy"])]
    steps_x = (1,) if layers == 2 else (1, -1)
    packed_rows = -(-tiles // 8) * 8
    slots = -(-len(gram_pairs(rhs)) // 8) * 8
    halves = -(-count // 2)

    message = shape(comps + halves, rows, lanes)
    blocks, edge, first, second = call(
        functools.partial(prepare_kernel, layers, rhs, comps),
        [shape(count, size, rows, lanes), shape(comps, rows, lanes), message, message],
        [start, raw],
        [pltpu.VMEM((2 * halves, rows, lanes), jnp.float32)],
    )
    first, second = (lax.ppermute(value, "gz", pairs) for value, pairs in zip((first, second), z_pairs))
    row_message = shape(packed_rows, lanes)
    field, *sent = call(
        functools.partial(assemble_kernel, rhs, comps),
        [shape(tiles * rows, lanes), row_message, row_message],
        [start, edge, first, second],
    )
    (ghosts,) = call(
        functools.partial(ghost_blocks_kernel, rhs, comps),
        [shape(count, size, rows, lanes)],
        [first, second],
        flops=4_000_000,
    )

    moved = pltpu.VMEM((count, tiles, rows, lanes), jnp.float32)
    basis, products = [start], []
    for step in range(STEPS):
        slabs = [field] + [
            lax.ppermute(field, ("gx", "gy"), across(sizes["gx"], by, still)) for by in steps_x
        ]
        heads, tails = (
            [lax.ppermute(value, ("gx", "gy"), across(sizes["gx"], by, pairs)) for by in (0, *steps_x)]
            for value, pairs in zip(sent, y_pairs)
        )
        last = step == STEPS - 1
        flops = 2 * count * comps * fields * rows * lanes
        if last:
            product, gram = call(
                functools.partial(operator_kernel, layers, rhs, comps, True),
                [shape(fields, rows, lanes), shape(devices, slots)],
                [blocks, *slabs, *heads, *tails, start, *products],
                [moved, pltpu.VMEM((slots * rows, lanes), jnp.float32)],
                flops,
            )
        else:
            product, field, *sent = call(
                functools.partial(operator_kernel, layers, rhs, comps, False),
                [shape(fields, rows, lanes), shape(tiles * rows, lanes), row_message, row_message],
                [blocks, ghosts, *slabs, *heads, *tails],
                [moved],
                flops,
            )
            basis.append(field)
        products.append(product)

    sums = lax.all_to_all(gram, AXES, 0, 0, tiled=True)
    answer, residual = call(
        functools.partial(finish_kernel, rhs, comps),
        [shape(fields, rows, lanes)] * 2,
        [sums, *basis, *products],
    )
    return answer.reshape(right_side.shape), residual.reshape(right_side.shape)


def solution(mesh):
    cells = P(None, None, "gx", "gy", "gz")
    return jax.shard_map(
        functools.partial(shards, dict(mesh.shape)),
        mesh=mesh,
        in_specs=(cells, P(None, None, None, "gx", "gy", "gz")),
        out_specs=(cells, cells),
        check_vma=False,
    )
```

```python
import functools

import jax
import jax.numpy as jnp
from jax import lax
from jax.experimental import pallas as pl
from jax.experimental.pallas import tpu as pltpu
from jax.sharding import PartitionSpec as P

STEPS = 3
CENTRE = 8.97
GROUP = 8
AXES = ("gx", "gy", "gz")

VMEM = pl.BlockSpec(memory_space=pltpu.VMEM)
HBM = pl.BlockSpec(memory_space=pltpu.HBM)


def call(body, outs, operands, scratch=(), flops=100_000, space=VMEM, limit=24 * 1024 * 1024):
    moved = sum(o.size * 4 for o in outs) + sum(o.size * o.dtype.itemsize for o in operands)
    return pl.pallas_call(
        body,
        out_shape=outs,
        in_specs=[space] * len(operands),
        out_specs=[VMEM] * len(outs),
        scratch_shapes=list(scratch),
        compiler_params=pltpu.CompilerParams(vmem_limit_bytes=limit),
        cost_estimate=pl.CostEstimate(flops=flops, bytes_accessed=moved, transcendentals=0),
    )(*operands)


def shape(*dims):
    return jax.ShapeDtypeStruct(dims, jnp.float32)


def lane_ids(rows, lanes):
    return lax.broadcasted_iota(jnp.int32, (rows, lanes), 1)


def row_ids(rows, lanes):
    return lax.broadcasted_iota(jnp.int32, (rows, lanes), 0)


def edge_tile(main, comp, rhs, comps, rows, lanes):
    lane = lane_ids(rows, lanes)
    place = lane % GROUP
    tile = jnp.zeros((rows, lanes), jnp.float32)
    for r in range(rhs):
        value = main(r * comps + comp)
        low = pltpu.roll(value, (r * GROUP + 3) % lanes, 1)
        high = pltpu.roll(value, (r * GROUP + 5) % lanes, 1)
        here = lane // GROUP == r
        tile = jnp.where(here & (place < 4), low, jnp.where(here, high, tile))
    return tile


def prepare_kernel(layers, comps, raw_hbm, *refs):
    blocks_refs = refs[:layers]
    first_ref, second_ref, raw_ref, narrow_ref, sem = refs[layers:]
    _, _, rows, lanes = raw_ref.shape
    size = comps * comps
    copies = []
    for i in range(9):
        copies.append(
            [pltpu.make_async_copy(raw_hbm.at[j], raw_ref.at[j], sem.at[j]) for j in (i, 9 + i, 18 + i)]
        )
        for copy in copies[i]:
            copy.start()

    lane = lane_ids(rows, lanes)
    pair = lane % 4 < 2
    zero = jnp.zeros((rows, lanes), jnp.float32)
    even = lax.axis_index("gz") % 2 == 0
    for i in range(9):
        for copy in copies[i]:
            copy.wait()
        tiles = [zero] * layers
        for at in range(size):
            below, own, above = (raw_ref[x * 9 + i, at].astype(jnp.float32) for x in range(3))
            found = [own, below + above] if layers == 2 else [own, below, above]
            for layer, block in enumerate(found):
                blocks_refs[layer][i, at] = block
                moved = pltpu.roll(block, (at * 4 + 2) % lanes, 1)
                tiles[layer] = jnp.where(lane // 4 == at, moved, tiles[layer])
        for layer in range(layers):
            narrow_ref[layer * 9 + i] = tiles[layer]
    if layers % 2:
        narrow_ref[9 * layers] = zero
    for i in range(0, narrow_ref.shape[0], 2):
        one, two = narrow_ref[i], narrow_ref[i + 1]
        up = jnp.where(pair, one, pltpu.roll(two, 2, 1))
        down = jnp.where(pair, pltpu.roll(one, lanes - 2, 1), two)
        first_ref[i // 2] = jnp.where(even, up, down)
        second_ref[i // 2] = jnp.where(even, down, up)


def message_kernel(rhs, comps, start_ref, one_ref, two_ref, edge_ref, first_ref, second_ref):
    _, rows, lanes = start_ref.shape
    for comp in range(comps):
        tile = edge_tile(lambda i: start_ref[i], comp, rhs, comps, rows, lanes)
        edge_ref[comp] = tile
        first_ref[comp] = tile
        second_ref[comp] = tile
    for i in range(one_ref.shape[0]):
        first_ref[comps + i] = one_ref[i]
        second_ref[comps + i] = two_ref[i]


def send_rows(field_ref, first_ref, second_ref, tiles, rows):
    even = lax.axis_index("gy") % 2 == 0
    head = field_ref[pl.ds(0, tiles, stride=rows), :]
    tail = field_ref[pl.ds(rows - 1, tiles, stride=rows), :]
    spare = first_ref.shape[0] - tiles
    if spare:
        empty = jnp.zeros((spare, first_ref.shape[1]), jnp.float32)
        first_ref[pl.ds(tiles, spare), :] = empty
        second_ref[pl.ds(tiles, spare), :] = empty
    first_ref[pl.ds(0, tiles), :] = jnp.where(even, tail, head)
    second_ref[pl.ds(0, tiles), :] = jnp.where(even, head, tail)


def assemble_kernel(rhs, comps, start_ref, edge_ref, first_ref, second_ref, out_ref, head_ref, tail_ref):
    fields, rows, lanes = start_ref.shape
    even = lax.axis_index("gz") % 2 == 0
    place = lane_ids(rows, lanes) % GROUP
    for i in range(fields):
        out_ref[pl.ds(i * rows, rows), :] = start_ref[i]
    for comp in range(comps):
        one, two = first_ref[comp], second_ref[comp]
        above = jnp.where(even, one, two)
        below = jnp.where(even, two, one)
        ghost = jnp.where(place < 3, below, jnp.where(place > 4, above, edge_ref[comp]))
        out_ref[pl.ds((fields + comp) * rows, rows), :] = ghost
    send_rows(out_ref, head_ref, tail_ref, fields + comps, rows)


def ghost_blocks_kernel(layers, rhs, comps, first_ref, second_ref, *out_refs):
    count, size, rows, lanes = out_refs[0].shape
    even = lax.axis_index("gz") % 2 == 0
    lane = lane_ids(rows, lanes)
    pair = lane % 4 < 2
    place = lane % GROUP
    column = jnp.where(place < 3, place - 1, place - 3)
    inner = (place == 1) | (place == 2) | (place == 5) | (place == 6)
    inner = inner & (lane < rhs * GROUP)
    total = count * layers
    for i in range(0, total, 2):
        one, two = first_ref[comps + i // 2], second_ref[comps + i // 2]
        above = jnp.where(even, one, two)
        below = jnp.where(even, two, one)
        tiles = [jnp.where(pair, below, pltpu.roll(above, 2, 1))]
        if i + 1 < total:
            tiles.append(jnp.where(pair, pltpu.roll(below, lanes - 2, 1), above))
        for at in range(size):
            index = jnp.where(inner, column + at * 4, lanes - 1)
            for k, tile in enumerate(tiles):
                layer, where = divmod(i + k, count)
                out_refs[layer][where, at] = jnp.take_along_axis(tile, index, axis=1)


def row_blocks_kernel(layers, *refs):
    block_refs, out_ref = refs[:layers], refs[layers]
    _, size, rows, lanes = out_ref.shape
    sub = row_ids(rows, lanes)

    def body(at, carry):
        for dz in range(3):
            tile = jnp.zeros((rows, lanes), jnp.float32)
            for layer in range(layers):
                low, high = block_refs[layer][dz, at], block_refs[layer][6 + dz, at]
                if layer:
                    low, high = pltpu.roll(low, layer, 0), pltpu.roll(high, rows - layer, 0)
                tile = jnp.where(sub == layer, low, jnp.where(sub == rows - 1 - layer, high, tile))
            out_ref[dz, at] = tile
        return carry

    lax.fori_loop(0, size, body, 0)


def accumulate(count, rhs, comps, ghosted, blocks, ghosts, value, total):
    fields = rhs * comps

    def body(at, total):
        total = list(total)
        for source in range(comps):
            values = [value(at, r * comps + source) for r in range(rhs)]
            for comp in range(comps):
                block = blocks[at, comp * comps + source]
                for r in range(rhs):
                    total[r * comps + comp] += block * values[r]
            if ghosted:
                ghost = value(at, fields + source)
                for comp in range(comps):
                    total[fields + comp] += ghosts[at, comp * comps + source] * ghost
        return tuple(total)

    return lax.fori_loop(0, count, body, tuple(total))


def interior_kernel(rhs, comps, ghosted, chained, *refs):
    fields, tiles = rhs * comps, (rhs + 1) * comps
    blocks_ref, field_ref, refs = refs[0], refs[1], refs[2:]
    ghosts_ref = before_ref = None
    if ghosted:
        ghosts_ref, refs = refs[0], refs[1:]
    if chained:
        before_ref, refs = refs[0], refs[1:]
    out_ref, moved_ref = refs
    _, _, rows, lanes = blocks_ref.shape
    sub, lane = row_ids(rows, lanes), lane_ids(rows, lanes)

    def spread(dz, tile, value):
        moved_ref[dz, tile] = jnp.where(sub == 0, 0.0, pltpu.roll(value, 1, 0))
        moved_ref[3 + dz, tile] = value
        moved_ref[6 + dz, tile] = jnp.where(sub == rows - 1, 0.0, pltpu.roll(value, rows - 1, 0))

    for comp in range(comps):
        ghost = field_ref[pl.ds((fields + comp) * rows, rows), :]
        if ghosted:
            spread(0, fields + comp, pltpu.roll(ghost, 1, 1))
            spread(1, fields + comp, ghost)
            spread(2, fields + comp, pltpu.roll(ghost, lanes - 1, 1))
        for r in range(rhs):
            tile = r * comps + comp
            value = field_ref[pl.ds(tile * rows, rows), :]
            left = pltpu.roll(ghost, (-(r * GROUP + 2)) % lanes, 1)
            right = pltpu.roll(ghost, (lanes - 1 - (r * GROUP + 5)) % lanes, 1)
            spread(0, tile, jnp.where(lane == 0, left, pltpu.roll(value, 1, 1)))
            spread(1, tile, value)
            spread(2, tile, jnp.where(lane == lanes - 1, right, pltpu.roll(value, lanes - 1, 1)))

    used = tiles if ghosted else fields
    zero = jnp.zeros((rows, lanes), jnp.float32)
    total = [before_ref[i] if chained else zero for i in range(used)]
    total = accumulate(
        9, rhs, comps, ghosted, blocks_ref, ghosts_ref, lambda at, tile: moved_ref[at, tile], total
    )
    for i in range(used):
        out_ref[i] = total[i]


def boundary_total(layers, rhs, comps, ghosted, rowblocks_ref, rowghosts_ref, heads, tails, interior_ref, packed_ref, ghost_ref, lines_ref):
    fields, tiles = rhs * comps, (rhs + 1) * comps
    _, _, rows, lanes = rowblocks_ref.shape
    even = lax.axis_index("gy") % 2 == 0
    lines = packed_ref.shape[0]
    zero = jnp.zeros((rows, lanes), jnp.float32)
    for dz in range(3):
        for tile in range(tiles):
            lines_ref[dz, pl.ds(tile * rows, rows), :] = zero
    for layer in range(layers):
        one, two = heads[layer][...], tails[layer][...]
        for line, packed in (
            (layer, jnp.where(even, two, one)),
            (rows - 1 - layer, jnp.where(even, one, two)),
        ):
            packed_ref[...] = packed
            for r in range(rhs):
                ghost_ref[pl.ds(r * comps, comps), :] = packed_ref[pl.ds(fields, comps), :]
            parts = [[], [], []]
            for top in range(0, lines, 8):
                part = packed[top : top + 8, :]
                sub, lane = row_ids(8, lanes) + top, lane_ids(8, lanes)
                low, high = pltpu.roll(part, 1, 1), pltpu.roll(part, lanes - 1, 1)
                if top < fields:
                    ghost = ghost_ref[pl.ds(top, 8), :]
                    group = jnp.minimum(sub // comps, rhs - 1) * GROUP
                    left = jnp.take_along_axis(ghost, group + 2, axis=1)
                    right = jnp.take_along_axis(ghost, group + 5, axis=1)
                    main = sub < fields
                    low = jnp.where(main & (lane == 0), left, low)
                    high = jnp.where(main & (lane == lanes - 1), right, high)
                for group, value in zip(parts, (low, part, high)):
                    group.append(value)
            for dz in range(3):
                value = jnp.concatenate(parts[dz], axis=0)[:tiles]
                lines_ref[dz, pl.ds(line, tiles, stride=rows), :] = value

    used = tiles if ghosted else fields
    added = accumulate(
        3, rhs, comps, ghosted, rowblocks_ref, rowghosts_ref,
        lambda at, tile: lines_ref[at, pl.ds(tile * rows, rows), :], [zero] * used,
    )
    sub = row_ids(rows, lanes)
    total = []
    for i in range(used):
        low = high = added[i]
        for layer in range(1, layers):
            low = low + pltpu.roll(added[i], rows - layer, 0)
            high = high + pltpu.roll(added[i], layer, 0)
        extra = jnp.where(sub == 0, low, jnp.where(sub == rows - 1, high, 0.0))
        total.append(interior_ref[i] + extra)
    return total


def advance_kernel(layers, rhs, comps, rowblocks_ref, rowghosts_ref, interior_ref, field_ref, *refs):
    fields, tiles = rhs * comps, (rhs + 1) * comps
    heads, tails = refs[:layers], refs[layers : 2 * layers]
    product_ref, next_ref, head_ref, tail_ref, *scratch = refs[2 * layers :]
    _, rows, lanes = interior_ref.shape
    total = boundary_total(
        layers, rhs, comps, True, rowblocks_ref, rowghosts_ref, heads, tails, interior_ref, *scratch
    )
    main = []
    for i in range(fields):
        product_ref[i] = total[i]
        main.append(total[i] - CENTRE * field_ref[pl.ds(i * rows, rows), :])
        next_ref[pl.ds(i * rows, rows), :] = main[i]
    place = lane_ids(rows, lanes) % GROUP
    own = (place == 3) | (place == 4)
    for comp in range(comps):
        where = pl.ds((fields + comp) * rows, rows)
        ghost = total[fields + comp] - CENTRE * field_ref[where, :]
        edge = edge_tile(lambda i: main[i], comp, rhs, comps, rows, lanes)
        next_ref[where, :] = jnp.where(own, edge, ghost)
    send_rows(next_ref, head_ref, tail_ref, tiles, rows)


def gram_pairs(rhs):
    size = rhs * STEPS
    pairs = [(i, j) for i in range(size) for j in range(i, size)]
    pairs += [(-1 - r, j) for r in range(rhs) for j in range(size)]
    known = size - rhs
    return [p for p in pairs if p[1] < known], [p for p in pairs if p[1] >= known]


def gram_row(pairs, offset, slots, rhs, comps, start_ref, products, pairs_ref):
    _, rows, lanes = start_ref.shape
    for at, (one, two) in enumerate(pairs):
        left = products[one // rhs] if one >= 0 else start_ref
        first = (one % rhs if one >= 0 else -1 - one) * comps
        second = two % rhs * comps
        accum = None
        for comp in range(comps):
            term = left[first + comp] * products[two // rhs][second + comp]
            accum = term if accum is None else accum + term
        pairs_ref[pl.ds(at * rows, rows), :] = accum
    count = pairs_ref.shape[0] // rows
    for at in range(len(pairs), count):
        pairs_ref[pl.ds(at * rows, rows), :] = jnp.zeros((rows, lanes), jnp.float32)
    sums = pairs_ref[pl.ds(0, count, stride=rows), :]
    for row in range(1, rows):
        sums = sums + pairs_ref[pl.ds(row, count, stride=rows), :]
    sums = jnp.sum(sums, axis=1, keepdims=True)
    diagonal = row_ids(count, slots) + offset == lane_ids(count, slots)
    return jnp.sum(jnp.where(diagonal, sums, 0.0), axis=0, keepdims=True)


def early_gram_kernel(rhs, comps, slots, start_ref, *refs):
    products, (out_ref, pairs_ref) = refs[: STEPS - 1], refs[STEPS - 1 :]
    early, _ = gram_pairs(rhs)
    row = gram_row(early, 0, slots, rhs, comps, start_ref, products, pairs_ref)
    out_ref[...] = jnp.broadcast_to(row, out_ref.shape)


def last_kernel(layers, rhs, comps, rowblocks_ref, interior_ref, early_ref, start_ref, *refs):
    fields = rhs * comps
    heads, tails, refs = refs[:layers], refs[layers : 2 * layers], refs[2 * layers :]
    products, refs = list(refs[: STEPS - 1]), refs[STEPS - 1 :]
    out_ref, gram_ref, pairs_ref, *scratch = refs
    total = boundary_total(
        layers, rhs, comps, False, rowblocks_ref, None, heads, tails, interior_ref, *scratch
    )
    for i in range(fields):
        out_ref[i] = total[i]
    early, late = gram_pairs(rhs)
    slots = gram_ref.shape[1]
    row = gram_row(late, len(early), slots, rhs, comps, start_ref, products + [out_ref], pairs_ref)
    gram_ref[...] = jnp.broadcast_to(row + early_ref[pl.ds(0, 1), :], gram_ref.shape)


def finish_kernel(rhs, comps, sums_ref, start_ref, *refs):
    products = refs[STEPS - 1 : 2 * STEPS - 1]
    solution_ref, residual_ref = refs[2 * STEPS - 1 :]
    _, rows, lanes = start_ref.shape
    size = rhs * STEPS

    def basis_tile(k, tile):
        if k < rhs:
            return start_ref[tile]
        return refs[k // rhs - 1][pl.ds(tile * rows, rows), :]

    packed = jnp.sum(sums_ref[...], axis=0, keepdims=True)
    gram, right = {}, {}
    early, late = gram_pairs(rhs)
    for at, (one, two) in enumerate(early + late):
        entry = jnp.broadcast_to(packed[:, at : at + 1], (rows, lanes))
        if one >= 0:
            gram[one, two] = entry
        else:
            right[two, -1 - one] = entry
    inverse = []
    for k in range(size):
        inverse.append(1.0 / gram[k, k])
        for i in range(k + 1, size):
            factor = gram[k, i] * inverse[k]
            for j in range(i, size):
                gram[i, j] = gram[i, j] - factor * gram[k, j]
            for r in range(rhs):
                right[i, r] = right[i, r] - factor * right[k, r]
    for r in range(rhs):
        weights = [None] * size
        for k in range(size - 1, -1, -1):
            accum = right[k, r]
            for j in range(k + 1, size):
                accum = accum - gram[k, j] * weights[j]
            weights[k] = accum * inverse[k]
        for comp in range(comps):
            answer = None
            image = None
            for k in range(size):
                tile = k % rhs * comps + comp
                one = weights[k] * basis_tile(k, tile)
                two = weights[k] * products[k // rhs][tile]
                answer = one if answer is None else answer + one
                image = two if image is None else image + two
            solution_ref[r * comps + comp] = answer
            residual_ref[r * comps + comp] = start_ref[r * comps + comp] - image


def paired(count, ring):
    first = [(i, i ^ 1) for i in range(count)]
    second = []
    for i in range(1, count - 1, 2):
        second += [(i, i + 1), (i + 1, i)]
    if ring and count > 2:
        second += [(count - 1, 0), (0, count - 1)]
    return first, second


def across(count_x, step_x, pairs):
    count_y = len(pairs)
    return [
        (x * count_y + one, (x + step_x) % count_x * count_y + two) for x in range(count_x) for one, two in pairs
    ]


def shards(sizes, right_side, jacobian):
    rhs, comps, _, rows, lanes = right_side.shape
    fields, tiles = rhs * comps, (rhs + 1) * comps
    size = comps * comps
    layers = 2 if sizes["gx"] == 2 else 3
    devices = sizes["gx"] * sizes["gy"] * sizes["gz"]

    z_pairs = paired(sizes["gz"], False)
    y_pairs = paired(sizes["gy"], True)
    still = [(i, i) for i in range(sizes["gy"])]
    steps_x = (1,) if layers == 2 else (1, -1)
    packed_rows = -(-tiles // 8) * 8
    early, late = gram_pairs(rhs)
    slots = -(-(len(early) + len(late)) // 128) * 128
    halves = -(-9 * layers // 2)

    message = shape(comps + halves, rows, lanes)
    block_shape = shape(9, size, rows, lanes)
    narrow = shape(halves, rows, lanes)
    start = right_side.reshape(fields, rows, lanes)
    *blocks, one, two = call(
        functools.partial(prepare_kernel, layers, comps),
        [*[block_shape] * layers, narrow, narrow],
        [jacobian.reshape(27, size, rows, lanes)],
        [
            pltpu.VMEM((27, size, rows, lanes), jnp.bfloat16),
            pltpu.VMEM((2 * halves, rows, lanes), jnp.float32),
            pltpu.SemaphoreType.DMA((27,)),
        ],
        space=HBM,
        limit=54_000_000,
    )
    edge, first, second = call(
        functools.partial(message_kernel, rhs, comps),
        [shape(comps, rows, lanes), message, message],
        [start, one, two],
    )
    second = lax.ppermute(second, "gz", z_pairs[1])
    first = lax.ppermute(first, "gz", z_pairs[0])
    row_message = shape(packed_rows, lanes)
    field, *sent = call(
        functools.partial(assemble_kernel, rhs, comps),
        [shape(tiles * rows, lanes), row_message, row_message],
        [start, edge, first, second],
    )
    ghosts = call(
        functools.partial(ghost_blocks_kernel, layers, rhs, comps),
        [block_shape] * layers,
        [first, second],
        flops=2_000_000,
    )
    row_blocks = [
        call(
            functools.partial(row_blocks_kernel, layers),
            [shape(3, size, rows, lanes)],
            one,
            flops=500_000,
        )[0]
        for one in (blocks, ghosts)
    ]

    moved = pltpu.VMEM((9, tiles, rows, lanes), jnp.float32)
    edges = [
        pltpu.VMEM((packed_rows, lanes), jnp.float32),
        pltpu.VMEM((packed_rows, lanes), jnp.float32),
        pltpu.VMEM((3, tiles * rows, lanes), jnp.float32),
    ]
    basis, products = [start], []
    for step in range(STEPS):
        last = step == STEPS - 1
        slabs = [field] + [
            lax.ppermute(field, ("gx", "gy"), across(sizes["gx"], by, still)) for by in steps_x
        ]
        heads, tails = (
            [lax.ppermute(value, ("gx", "gy"), across(sizes["gx"], by, pairs)) for by in (0, *steps_x)]
            for value, pairs in zip(sent, y_pairs)
        )
        interior = None
        for layer in range(layers):
            operands = [blocks[layer], slabs[layer]]
            operands += [] if last else [ghosts[layer]]
            operands += [] if interior is None else [interior]
            (interior,) = call(
                functools.partial(interior_kernel, rhs, comps, not last, interior is not None),
                [shape(fields if last else tiles, rows, lanes)],
                operands,
                [moved],
                flops=2_000_000,
            )
        if last:
            (known,) = call(
                functools.partial(early_gram_kernel, rhs, comps, slots),
                [shape(8, slots)],
                [start, *products],
                [pltpu.VMEM((-(-len(early) // 8) * 8 * rows, lanes), jnp.float32)],
                flops=500_000,
            )
            product, gram = call(
                functools.partial(last_kernel, layers, rhs, comps),
                [shape(fields, rows, lanes), shape(devices, slots)],
                [row_blocks[0], interior, known, start, *heads, *tails, *products],
                [pltpu.VMEM((-(-len(late) // 8) * 8 * rows, lanes), jnp.float32), *edges],
            )
        else:
            product, field, *sent = call(
                functools.partial(advance_kernel, layers, rhs, comps),
                [shape(fields, rows, lanes), shape(tiles * rows, lanes), row_message, row_message],
                [*row_blocks, interior, field, *heads, *tails],
                edges,
            )
            basis.append(field)
        products.append(product)

    sums = lax.all_to_all(gram, AXES, 0, 0, tiled=True)
    answer, residual = call(
        functools.partial(finish_kernel, rhs, comps),
        [shape(fields, rows, lanes)] * 2,
        [sums, *basis, *products],
    )
    return answer.reshape(right_side.shape), residual.reshape(right_side.shape)


def solution(mesh):
    cells = P(None, None, "gx", "gy", "gz")
    return jax.shard_map(
        functools.partial(shards, dict(mesh.shape)),
        mesh=mesh,
        in_specs=(cells, P(None, None, None, "gx", "gy", "gz")),
        out_specs=(cells, cells),
        check_vma=False,
    )
```
